512 devices in a mesh: group: 2 (over y), seq: 16 (over z), batch: 8 (over x), head: 2 (over core).
Axes of the slice: x: 8, y: 2, z: 16, core: 2. Of those that a mesh axis runs over, the one named last changes fastest.
The devices are a block of a 8x8x16 slice.
Arguments:
- queries: bfloat16 [32, 4, 128, 576], P(('group', 'batch'), None, ('seq', 'head')), parts along dimension 0, may hold values from -40 to 40
- cache: bfloat16 [32, 32768, 576], P(('group', 'batch'), 'seq'), parts along dimension 0, may hold values from -6 to 6
- lengths: int32 [32], P(('group', 'batch')), parts along dimension 0, may hold values from 5 to 32768, as said below
Outputs:
- attended: bfloat16 [32, 4, 128, 512], P(('group', 'batch'), None, ('seq', 'head')), parts along dimension 0
The draws below stay inside these ranges and needn't reach their ends.
There are 2 independent parts, one for each index of `group`. The reference program is written for one: setup_inputs(seed, part) draws one part's arguments, and reference() takes and returns one part's arrays. A program takes and returns all parts, laid end to end along the dimension named above; each array names one. Nothing has to cross between parts.
Inputs may be any that keep to these rules, and one draw needn't show every extreme that they name: `lengths`: at least one sequence has length exactly 32768.
All inputs are finite; a program needn't handle non-finite values.
Results may differ from the reference program's by a relative error of at most 0.0065.
Values may be sent and summed in bfloat16 or wider, within the bound.
No kernel may reach another device: no remote copies, remote signals or barrier semaphores. Data moves between devices by JAX's collectives and lax.ppermute only.
A program may use at most 64 MiB of HBM per device.

```python
import jax
import jax.numpy as jnp
from jax import lax

H = 128
LAT = 512
ROPE = 64
NOPE = 128
DRAFT = 4
TOK_DEV = 2048
KDIM = 576
B = 16
CTX = 32768


def cache_base(key):
    first = jax.random.fold_in(key, 0)
    base = jnp.clip(jax.random.normal(first, (B, CTX, KDIM), jnp.float32), -6.0, 6.0)
    return base


def draw_cache(key, part):
    return cache_base(jax.random.fold_in(key, 11)).astype(jnp.bfloat16)


def draw_queries(key, part):
    first = jax.random.fold_in(jax.random.fold_in(key, 23), 0)
    values = 1.5 * jnp.clip(jax.random.normal(first, (B, DRAFT, H, KDIM), jnp.float32), -6.0, 6.0)
    return values.astype(jnp.bfloat16)


def draw_lengths(key, part):
    first, second, third, fourth = jax.random.split(jax.random.fold_in(key, 37), 4)
    spread = jax.random.randint(first, (B,), DRAFT + 1, CTX + 1)
    longer = jax.random.randint(second, (B,), CTX - TOK_DEV, CTX + 1)
    coin = jax.random.randint(third, (B,), 0, 2)
    chosen = jax.random.randint(fourth, (), 0, B)
    result = jnp.where(coin == 1, longer, spread)
    result = jnp.where(jnp.arange(B, dtype=jnp.int32) == chosen, CTX, result)
    return result.astype(jnp.int32)


def setup_inputs(seed: int = 0, part: int = 0) -> dict:
    streams_of = jax.random.split(jax.random.key(seed), 4)
    own_keys = jax.random.split(jax.random.fold_in(streams_of[3], part), 4)
    queries = draw_queries(jax.random.fold_in(jax.random.fold_in(streams_of[3], part), 71), part)
    cache = draw_cache(jax.random.fold_in(jax.random.fold_in(streams_of[3], part), 71), part)
    lengths = draw_lengths(jax.random.fold_in(jax.random.fold_in(streams_of[3], part), 71), part)
    return dict(queries=queries, cache=cache, lengths=lengths)


def attend_sequence(items):
    query_rows, keys, length = items
    scale = (NOPE + ROPE) ** -0.5
    scores = jnp.einsum("dhk,tk->dht", query_rows.astype(jnp.float32), keys.astype(jnp.float32)) * scale
    limit = length - DRAFT + jnp.arange(DRAFT, dtype=jnp.int32)
    visible = jnp.arange(CTX, dtype=jnp.int32)[None, None, :] <= limit[:, None, None]
    masked = jnp.where(visible, scores, jnp.float32(-1e30))
    peak = jnp.max(masked, axis=2)
    weights = jnp.where(visible, jnp.exp(masked - peak[:, :, None]), jnp.float32(0.0))
    total = jnp.sum(weights, axis=2)
    rounded = weights.astype(jnp.bfloat16).astype(jnp.float32)
    numerator = jnp.einsum("dht,tl->dhl", rounded, keys[:, :LAT].astype(jnp.float32))
    return (numerator / total[:, :, None]).astype(jnp.bfloat16)


def reference(queries, cache, lengths):
    return lax.map(attend_sequence, (queries, cache, lengths.astype(jnp.int32)))
```

```python
import functools
import math

import jax
import jax.numpy as jnp
from jax import lax
from jax.experimental import pallas as pl
from jax.experimental.pallas import tpu as pltpu
from jax.sharding import PartitionSpec as P

LAT = 512
ROPE = 64
NOPE = 128
LANES = 128
STAT_ROWS = 8
HIDDEN = -1e30
FLOOR = -1e25


def attend_kernel(chunk, seqs, draft, heads, peers, lengths_ref, first_ref, q_hbm, cache_hbm, out_ref,
                  q_vmem, k_vmem, s_vmem, q_sem, k_sem):
    tokens = cache_hbm.shape[1]
    chunks = tokens // chunk
    own = draft * heads
    rows = peers * own
    q_copy = pltpu.make_async_copy(q_hbm, q_vmem, q_sem)
    q_copy.start()
    copies = {}
    for b in range(seqs):
        for c in range(chunks):
            part = pl.ds(c * chunk, chunk)
            copies[b, c] = pltpu.make_async_copy(cache_hbm.at[b, part], k_vmem.at[b, part], k_sem.at[b, c])
            copies[b, c].start()
    q_copy.wait()
    scale = (NOPE + ROPE) ** (-0.5) * math.log2(math.e)
    row = lax.broadcasted_iota(jnp.int32, (rows, 1), 0)
    member = (row // heads) % draft
    lane = lax.broadcasted_iota(jnp.int32, (rows, LANES), 1)
    stats = jnp.zeros((rows, LANES), jnp.float32)
    first = first_ref[0]
    for b in range(seqs):
        q = q_vmem[:, b].reshape(rows, q_vmem.shape[-1])
        limit = lengths_ref[b] - draft - first + member
        tops = None
        for c in range(chunks):
            copies[b, c].wait()
            keys = k_vmem[b, c * chunk : (c + 1) * chunk]
            s = lax.dot_general(q, keys, (((1,), (1,)), ((), ())), preferred_element_type=jnp.float32)
            at = c * chunk + lax.broadcasted_iota(jnp.int32, (rows, chunk), 1)
            s = jnp.where(at <= limit, s * scale, HIDDEN)
            s_vmem[b, :, c * chunk : (c + 1) * chunk] = s
            for i in range(chunk // LANES):
                tile = s[:, i * LANES : (i + 1) * LANES]
                tops = tile if tops is None else jnp.maximum(tops, tile)
        peak = jnp.maximum(jnp.max(tops, axis=1, keepdims=True), FLOOR)
        point = peak.astype(jnp.bfloat16).astype(jnp.float32)
        sums = jnp.zeros((rows, LANES), jnp.float32)
        numerator = jnp.zeros((rows, LAT), jnp.float32)
        for c in range(chunks):
            w = jnp.exp2(s_vmem[b, :, c * chunk : (c + 1) * chunk] - point)
            for i in range(chunk // LANES):
                sums = sums + w[:, i * LANES : (i + 1) * LANES]
            values = k_vmem[b, c * chunk : (c + 1) * chunk, :LAT]
            numerator = numerator + jnp.dot(w.astype(jnp.bfloat16), values, preferred_element_type=jnp.float32)
        total = jnp.sum(sums, axis=1, keepdims=True)
        inverse = jnp.where(total > 0.0, 1.0 / total, 0.0)
        part = (numerator * inverse).astype(jnp.bfloat16)
        for i in range(LAT // LANES):
            tile = part[:, i * LANES : (i + 1) * LANES].reshape(peers, own, LANES)
            at = (i * seqs + b) * own
            out_ref[:, at : at + own, :] = tile
        high = total.astype(jnp.bfloat16).astype(jnp.float32)
        for i, value in enumerate((point, high, total - high)):
            stats = jnp.where(lane == 4 * b + i, value, stats)
    across = stats.T[:STAT_ROWS]
    base = seqs * own * (LAT // LANES)
    for p in range(peers):
        tile, at = divmod(p * own, LANES)
        mine = across[:, tile * LANES : (tile + 1) * LANES]
        if at:
            mine = pltpu.roll(mine, LANES - at, 1)
        out_ref[p, base : base + STAT_ROWS, :] = mine.astype(jnp.bfloat16)


def combine_kernel(seqs, draft, heads, peers, in_ref, out_ref):
    own = draft * heads
    base = seqs * own * (LAT // LANES)
    for b in range(seqs):
        stat = [in_ref[:, base + 4 * b + i, :].astype(jnp.float32) for i in range(3)]
        point, total = stat[0], stat[1] + stat[2]
        weight = total * jnp.exp2(point - jnp.max(point, axis=0, keepdims=True))
        weight = weight / jnp.sum(weight, axis=0, keepdims=True)
        column = jnp.concatenate([weight, jnp.zeros((LANES - peers, LANES), jnp.float32)], axis=0).T[:own]
        for i in range(LAT // LANES):
            at = (i * seqs + b) * own
            acc = jnp.zeros((own, LANES), jnp.float32)
            for p in range(peers):
                acc = acc + column[:, p : p + 1] * in_ref[p, at : at + own, :].astype(jnp.float32)
            out_ref[b, :, :, i * LANES : (i + 1) * LANES] = (
                acc.reshape(draft, heads, LANES).astype(jnp.bfloat16)
            )


def body(queries, cache, lengths):
    seqs, draft, heads, width = queries.shape
    tokens = cache.shape[1]
    peers = lax.axis_size("seq")
    own = draft * heads
    rows = peers * own
    chunk = 512
    message = seqs * own * (LAT // LANES) + STAT_ROWS
    everyone = lax.all_gather(queries.reshape(seqs, own, width), "seq", axis=0)
    first = (lax.axis_index("seq") * tokens).astype(jnp.int32).reshape(1)
    any_spec = pl.BlockSpec(memory_space=pl.ANY)
    smem = pl.BlockSpec(memory_space=pltpu.SMEM)
    partial = pl.pallas_call(
        functools.partial(attend_kernel, chunk, seqs, draft, heads, peers),
        out_shape=jax.ShapeDtypeStruct((peers, message, LANES), jnp.bfloat16),
        in_specs=[smem, smem, any_spec, any_spec],
        out_specs=pl.BlockSpec(memory_space=pltpu.VMEM),
        scratch_shapes=[
            pltpu.VMEM((peers, seqs, own, width), jnp.bfloat16),
            pltpu.VMEM((seqs, tokens, width), jnp.bfloat16),
            pltpu.VMEM((seqs, rows, tokens), jnp.float32),
            pltpu.SemaphoreType.DMA,
            pltpu.SemaphoreType.DMA((seqs, tokens // chunk)),
        ],
        name="attend",
    )(lengths, first, everyone, cache)
    arrived = lax.all_to_all(partial, "seq", split_axis=0, concat_axis=0, tiled=True)
    return pl.pallas_call(
        functools.partial(combine_kernel, seqs, draft, heads, peers),
        out_shape=jax.ShapeDtypeStruct((seqs, draft, heads, LAT), jnp.bfloat16),
        in_specs=[pl.BlockSpec(memory_space=pltpu.VMEM)],
        out_specs=pl.BlockSpec(memory_space=pltpu.VMEM),
        name="combine",
    )(arrived)


def solution(mesh):
    return jax.shard_map(
        body,
        mesh=mesh,
        in_specs=(
            P(("group", "batch"), None, ("seq", "head"), None),
            P(("group", "batch"), "seq", None),
            P(("group", "batch")),
        ),
        out_specs=P(("group", "batch"), None, ("seq", "head"), None),
        check_vma=False,
    )
```

```python
import functools
import math

import jax
import jax.numpy as jnp
from jax import lax
from jax.experimental import pallas as pl
from jax.experimental.pallas import tpu as pltpu
from jax.sharding import PartitionSpec as P

LAT = 512
ROPE = 64
NOPE = 128
LANES = 128
STAT_ROWS = 8
HIDDEN = -1e30
FLOOR = -1e25


def pack_kernel(seqs, q_ref, out_ref):
    own = q_ref.shape[1] * q_ref.shape[2]
    for b in range(seqs):
        q = q_ref[b].reshape(own, q_ref.shape[-1])
        for i in range(LAT // LANES):
            at = (i * seqs + b) * own
            out_ref[at : at + own, :] = q[:, i * LANES : (i + 1) * LANES]
        out_ref[LAT // LANES * seqs * own :, b * ROPE : (b + 1) * ROPE] = q[:, LAT:]


def attend_kernel(chunk, seqs, draft, heads, order, lengths_ref, q_ref, k_ref, out_ref, s_vmem):
    tokens = k_ref.shape[2]
    chunks = tokens // chunk
    own = draft * heads
    peers = len(order)
    rows = peers * own
    tiles = LAT // LANES
    scale = (NOPE + ROPE) ** (-0.5) * math.log2(math.e)
    row = lax.broadcasted_iota(jnp.int32, (rows, 1), 0)
    member = (row // heads) % draft
    lane = lax.broadcasted_iota(jnp.int32, (rows, LANES), 1)
    stats = jnp.zeros((rows, LANES), jnp.float32)
    for b in range(seqs):
        pieces = [
            q_ref[:, (i * seqs + b) * own : (i * seqs + b + 1) * own, :].reshape(rows, LANES) for i in range(tiles)
        ]
        rotary = q_ref[:, tiles * seqs * own :, :].reshape(rows, LANES)
        q = jnp.concatenate(pieces + [rotary[:, b * ROPE : (b + 1) * ROPE]], axis=1)
        limit = lengths_ref[b] - draft - lax.axis_index("seq") * tokens + member
        tops = None
        for c in range(chunks):
            keys = k_ref[b, :, c * chunk : (c + 1) * chunk]
            s = jnp.dot(q, keys, preferred_element_type=jnp.float32)
            at = c * chunk + lax.broadcasted_iota(jnp.int32, (rows, chunk), 1)
            s = jnp.where(at <= limit, s * scale, HIDDEN)
            s_vmem[b, :, c * chunk : (c + 1) * chunk] = s
            for i in range(chunk // LANES):
                tile = s[:, i * LANES : (i + 1) * LANES]
                tops = tile if tops is None else jnp.maximum(tops, tile)
        peak = jnp.maximum(jnp.max(tops, axis=1, keepdims=True), FLOOR)
        point = peak.astype(jnp.bfloat16).astype(jnp.float32)
        sums = jnp.zeros((rows, LANES), jnp.float32)
        numerator = jnp.zeros((rows, LAT), jnp.float32)
        for c in range(chunks):
            w = jnp.exp2(s_vmem[b, :, c * chunk : (c + 1) * chunk] - point)
            for i in range(chunk // LANES):
                sums = sums + w[:, i * LANES : (i + 1) * LANES]
            values = k_ref[b, :LAT, c * chunk : (c + 1) * chunk]
            numerator = numerator + lax.dot_general(
                w.astype(jnp.bfloat16), values, (((1,), (1,)), ((), ())), preferred_element_type=jnp.float32
            )
        total = jnp.sum(sums, axis=1, keepdims=True)
        inverse = jnp.where(total > 0.0, 1.0 / total, 0.0)
        part = (numerator * inverse).astype(jnp.bfloat16)
        for i in range(tiles):
            at = (i * seqs + b) * own
            for slot, p in enumerate(order):
                out_ref[p, at : at + own, :] = part[slot * own : (slot + 1) * own, i * LANES : (i + 1) * LANES]
        high = total.astype(jnp.bfloat16).astype(jnp.float32)
        for i, value in enumerate((point, high, total - high)):
            stats = jnp.where(lane == 4 * b + i, value, stats)
    across = stats.T[:STAT_ROWS]
    base = seqs * own * tiles
    for slot, p in enumerate(order):
        tile, at = divmod(slot * own, LANES)
        mine = across[:, tile * LANES : (tile + 1) * LANES]
        if at:
            mine = pltpu.roll(mine, LANES - at, 1)
        out_ref[p, base : base + STAT_ROWS, :] = mine.astype(jnp.bfloat16)


def combine_kernel(seqs, draft, heads, peers, in_ref, out_ref):
    own = draft * heads
    base = seqs * own * (LAT // LANES)
    for b in range(seqs):
        stat = [in_ref[:, base + 4 * b + i, :].astype(jnp.float32) for i in range(3)]
        point, total = stat[0], stat[1] + stat[2]
        weight = total * jnp.exp2(point - jnp.max(point, axis=0, keepdims=True))
        weight = weight / jnp.sum(weight, axis=0, keepdims=True)
        column = jnp.concatenate([weight, jnp.zeros((LANES - peers, LANES), jnp.float32)], axis=0).T[:own]
        for i in range(LAT // LANES):
            at = (i * seqs + b) * own
            acc = jnp.zeros((own, LANES), jnp.float32)
            for p in range(peers):
                acc = acc + column[:, p : p + 1] * in_ref[p, at : at + own, :].astype(jnp.float32)
            out_ref[b, :, :, i * LANES : (i + 1) * LANES] = (
                acc.reshape(draft, heads, LANES).astype(jnp.bfloat16)
            )


def body(queries, cache, lengths):
    seqs, draft, heads, width = queries.shape
    tokens = cache.shape[1]
    peers = lax.axis_size("seq")
    own = draft * heads
    rows = peers * own
    chunk = 512
    packed = seqs * own * width // LANES
    message = seqs * own * (LAT // LANES) + STAT_ROWS
    vmem = pl.BlockSpec(memory_space=pltpu.VMEM)
    smem = pl.BlockSpec(memory_space=pltpu.SMEM)
    mine = pl.pallas_call(
        functools.partial(pack_kernel, seqs),
        out_shape=jax.ShapeDtypeStruct((packed, LANES), jnp.bfloat16),
        in_specs=[vmem],
        out_specs=vmem,
        cost_estimate=pl.CostEstimate(flops=5_000_000_000, bytes_accessed=150_000, transcendentals=0),
        compiler_params=pltpu.CompilerParams(vmem_limit_bytes=4 * 1024 * 1024),
        name="pack",
    )(queries)
    everyone = lax.all_gather(mine, "seq", axis=0)
    partial = pl.pallas_call(
        functools.partial(attend_kernel, chunk, seqs, draft, heads, list(range(peers))),
        out_shape=jax.ShapeDtypeStruct((peers, message, LANES), jnp.bfloat16),
        in_specs=[smem, vmem, vmem],
        out_specs=vmem,
        scratch_shapes=[pltpu.VMEM((seqs, rows, tokens), jnp.float32)],
        compiler_params=pltpu.CompilerParams(vmem_limit_bytes=24 * 1024 * 1024),
        name="attend",
    )(lengths, everyone, jnp.swapaxes(cache, 1, 2))
    arrived = lax.all_to_all(partial, "seq", split_axis=0, concat_axis=0, tiled=True)
    return pl.pallas_call(
        functools.partial(combine_kernel, seqs, draft, heads, peers),
        out_shape=jax.ShapeDtypeStruct((seqs, draft, heads, LAT), jnp.bfloat16),
        in_specs=[vmem],
        out_specs=vmem,
        compiler_params=pltpu.CompilerParams(vmem_limit_bytes=8 * 1024 * 1024),
        name="combine",
    )(arrived)


def solution(mesh):
    return jax.shard_map(
        body,
        mesh=mesh,
        in_specs=(
            P(("group", "batch"), None, ("seq", "head"), None),
            P(("group", "batch"), "seq", None),
            P(("group", "batch")),
        ),
        out_specs=P(("group", "batch"), None, ("seq", "head"), None),
        check_vma=False,
    )
```

```python
import functools
import math

import jax
import jax.numpy as jnp
from jax import lax
from jax.experimental import pallas as pl
from jax.experimental.pallas import tpu as pltpu
from jax.sharding import PartitionSpec as P

LAT = 512
ROPE = 64
NOPE = 128
LANES = 128
STAT_ROWS = 8
HIDDEN = -1e30
FLOOR = -1e25


def pack_kernel(seqs, q_ref, out_ref):
    own = q_ref.shape[1] * q_ref.shape[2]
    for b in range(seqs):
        q = q_ref[b].reshape(own, q_ref.shape[-1])
        for i in range(LAT // LANES):
            at = (i * seqs + b) * own
            out_ref[at : at + own, :] = q[:, i * LANES : (i + 1) * LANES]
        out_ref[LAT // LANES * seqs * own :, b * ROPE : (b + 1) * ROPE] = q[:, LAT:]


def attend_kernel(chunk, seqs, draft, heads, order, lengths_ref, q_ref, k_ref, out_ref, s_vmem):
    tokens = k_ref.shape[2]
    chunks = tokens // chunk
    own = draft * heads
    peers = len(order)
    rows = peers * own
    tiles = LAT // LANES
    scale = (NOPE + ROPE) ** (-0.5) * math.log2(math.e)
    row = lax.broadcasted_iota(jnp.int32, (rows, 1), 0)
    member = (row // heads) % draft
    lane = lax.broadcasted_iota(jnp.int32, (rows, LANES), 1)
    stats = jnp.zeros((rows, LANES), jnp.float32)
    highs = []
    for b in range(seqs):
        pieces = [
            q_ref[:, (i * seqs + b) * own : (i * seqs + b + 1) * own, :].reshape(rows, LANES) for i in range(tiles)
        ]
        rotary = q_ref[:, tiles * seqs * own :, :].reshape(rows, LANES)
        q = jnp.concatenate(pieces + [rotary[:, b * ROPE : (b + 1) * ROPE]], axis=1)
        limit = lengths_ref[b] - draft - lax.axis_index("seq") * tokens + member
        tops = None
        for c in range(chunks):
            keys = k_ref[b, :, c * chunk : (c + 1) * chunk]
            s = jnp.dot(q, keys, preferred_element_type=jnp.float32)
            at = c * chunk + lax.broadcasted_iota(jnp.int32, (rows, chunk), 1)
            s = jnp.where(at <= limit, s * scale, HIDDEN)
            s_vmem[b, :, c * chunk : (c + 1) * chunk] = s
            for i in range(chunk // LANES):
                tile = s[:, i * LANES : (i + 1) * LANES]
                tops = tile if tops is None else jnp.maximum(tops, tile)
        highs.append(tops)
    for b in range(seqs):
        peak = jnp.maximum(jnp.max(highs[b], axis=1, keepdims=True), FLOOR)
        point = peak.astype(jnp.bfloat16).astype(jnp.float32)
        sums = jnp.zeros((rows, LANES), jnp.float32)
        numerator = jnp.zeros((rows, LAT), jnp.float32)
        for c in range(chunks):
            w = jnp.exp2(s_vmem[b, :, c * chunk : (c + 1) * chunk] - point)
            for i in range(chunk // LANES):
                sums = sums + w[:, i * LANES : (i + 1) * LANES]
            values = k_ref[b, :LAT, c * chunk : (c + 1) * chunk]
            numerator = numerator + lax.dot_general(
                w.astype(jnp.bfloat16), values, (((1,), (1,)), ((), ())), preferred_element_type=jnp.float32
            )
        total = jnp.sum(sums, axis=1, keepdims=True)
        inverse = jnp.where(total > 0.0, 1.0 / total, 0.0)
        part = (numerator * inverse).astype(jnp.bfloat16)
        for i in range(tiles):
            at = (i * seqs + b) * own
            for slot, p in enumerate(order):
                out_ref[p, at : at + own, :] = part[slot * own : (slot + 1) * own, i * LANES : (i + 1) * LANES]
        high = total.astype(jnp.bfloat16).astype(jnp.float32)
        for i, value in enumerate((point, high, total - high)):
            stats = jnp.where(lane == 4 * b + i, value, stats)
    across = stats.T[:STAT_ROWS]
    base = seqs * own * tiles
    for slot, p in enumerate(order):
        tile, at = divmod(slot * own, LANES)
        mine = across[:, tile * LANES : (tile + 1) * LANES]
        if at:
            mine = pltpu.roll(mine, LANES - at, 1)
        out_ref[p, base : base + STAT_ROWS, :] = mine.astype(jnp.bfloat16)


def combine_kernel(seqs, draft, heads, peers, in_ref, out_ref):
    own = draft * heads
    base = seqs * own * (LAT // LANES)
    for b in range(seqs):
        stat = [in_ref[:, base + 4 * b + i, :].astype(jnp.float32) for i in range(3)]
        point, total = stat[0], stat[1] + stat[2]
        weight = total * jnp.exp2(point - jnp.max(point, axis=0, keepdims=True))
        weight = weight / jnp.sum(weight, axis=0, keepdims=True)
        column = jnp.concatenate([weight, jnp.zeros((LANES - peers, LANES), jnp.float32)], axis=0).T[:own]
        for i in range(LAT // LANES):
            at = (i * seqs + b) * own
            acc = jnp.zeros((own, LANES), jnp.float32)
            for p in range(peers):
                acc = acc + column[:, p : p + 1] * in_ref[p, at : at + own, :].astype(jnp.float32)
            out_ref[b, :, :, i * LANES : (i + 1) * LANES] = (
                acc.reshape(draft, heads, LANES).astype(jnp.bfloat16)
            )


def body(queries, cache, lengths):
    seqs, draft, heads, width = queries.shape
    tokens = cache.shape[1]
    peers = lax.axis_size("seq")
    own = draft * heads
    rows = peers * own
    chunk = 1024
    packed = seqs * own * width // LANES
    message = seqs * own * (LAT // LANES) + STAT_ROWS
    vmem = pl.BlockSpec(memory_space=pltpu.VMEM)
    smem = pl.BlockSpec(memory_space=pltpu.SMEM)
    mine = pl.pallas_call(
        functools.partial(pack_kernel, seqs),
        out_shape=jax.ShapeDtypeStruct((packed, LANES), jnp.bfloat16),
        in_specs=[vmem],
        out_specs=vmem,
        cost_estimate=pl.CostEstimate(flops=5_000_000_000, bytes_accessed=150_000, transcendentals=0),
        compiler_params=pltpu.CompilerParams(vmem_limit_bytes=4 * 1024 * 1024),
        name="pack",
    )(queries)
    everyone = lax.all_gather(mine, "seq", axis=0)
    partial = pl.pallas_call(
        functools.partial(attend_kernel, chunk, seqs, draft, heads, list(range(peers))),
        out_shape=jax.ShapeDtypeStruct((peers, message, LANES), jnp.bfloat16),
        in_specs=[smem, vmem, vmem],
        out_specs=vmem,
        scratch_shapes=[pltpu.VMEM((seqs, rows, tokens), jnp.float32)],
        compiler_params=pltpu.CompilerParams(vmem_limit_bytes=24 * 1024 * 1024),
        name="attend",
    )(lengths, everyone, jnp.swapaxes(cache, 1, 2))
    arrived = lax.all_to_all(partial, "seq", split_axis=0, concat_axis=0, tiled=True)
    return pl.pallas_call(
        functools.partial(combine_kernel, seqs, draft, heads, peers),
        out_shape=jax.ShapeDtypeStruct((seqs, draft, heads, LAT), jnp.bfloat16),
        in_specs=[vmem],
        out_specs=vmem,
        compiler_params=pltpu.CompilerParams(vmem_limit_bytes=8 * 1024 * 1024),
        name="combine",
    )(arrived)


def solution(mesh):
    return jax.shard_map(
        body,
        mesh=mesh,
        in_specs=(
            P(("group", "batch"), None, ("seq", "head"), None),
            P(("group", "batch"), "seq", None),
            P(("group", "batch")),
        ),
        out_specs=P(("group", "batch"), None, ("seq", "head"), None),
        check_vma=False,
    )
```
